256 devices in a mesh: expert: 8 (over z), neuron: 32 (over y, x, core).
Axes of the slice: x: 4, y: 4, z: 8, core: 2. Of those that a mesh axis runs over, the one named last changes fastest.
Arguments:
- tokens: bfloat16 [1024, 4096], P('neuron'), may hold values from -6 to 6
- route_logits: float32 [1024, 2], replicated, may hold values from -6 to 6
- expert_ids: int32 [1024, 2], replicated, may hold values from 0 to 7, all different within a row; in each aligned block of 1024 rows (0 to 1023, 1024 to 2047, ...) at most 512 rows name the same one
- block_live: int32 [8, 224], P('expert', 'neuron'), may hold values 0 or 1
- w_gate: bfloat16 [8, 4096, 14336], P('expert', None, 'neuron'), may hold values from -0.09375 to 0.09375
- w_up: bfloat16 [8, 4096, 14336], P('expert', None, 'neuron'), may hold values from -0.09375 to 0.09375
- w_down: bfloat16 [8, 14336, 4096], P('expert', 'neuron'), may hold values from -0.046875 to 0.046875
Outputs:
- mixed: bfloat16 [1024, 4096], P('neuron')
The draws below stay inside these ranges and needn't reach their ends.
Inputs may be any that keep to these rules, and one draw needn't show every extreme that they name: `expert_ids`: each token names two different experts; no expert is named by more than 512 tokens, a bound that some block reaches; every expert is named.
All inputs are finite; a program needn't handle non-finite values. No bound on the sum of `block_live` on one device may be relied on, other than what follows from the above.
Results may differ from the reference program's by a relative error of at most 0.0049.
Values may be sent and summed in bfloat16 or wider, within the bound.
No kernel may reach another device: no remote copies, remote signals or barrier semaphores. Data moves between devices by JAX's collectives and lax.ppermute only.
A program may use at most 128 MiB of HBM per device.

```python
import math
import jax
import jax.numpy as jnp
import numpy as np
from jax import lax

D = 4096
FF = 14336
TOP = 2
BLK = 64
EXPERTS = 8
TOKENS = 1024
CAP = 512


def place_ends(values, rng, low, high):
    place = [jax.random.randint(jax.random.fold_in(rng, axis), (), 0, length) for axis, length in enumerate(values.shape)]
    main_axis = values.shape.index(max(values.shape))
    neighbour = place[:main_axis] + [(place[main_axis] + 1) % values.shape[main_axis]] + place[main_axis + 1:]
    return values.at[tuple(place)].set(low).at[tuple(neighbour)].set(high)


def steps_of(key, shape, pieces, low, high):
    def one(position, blocks):
        draws = jax.random.uniform(jax.random.fold_in(jax.random.fold_in(key, 6), position), (blocks,), jnp.float32, low / len(pieces), high / len(pieces))
        return jnp.repeat(jnp.exp(draws), shape[position] // blocks).reshape((-1,) + (1,) * (len(shape) - position - 1))

    loudness = one(*pieces[0])
    for cut in pieces[1:]:
        loudness = loudness * one(*cut)
    return loudness


def assign_block(key, own, number, rows, count, top, limit, slope):
    ranking = jax.random.permutation(key, count)
    heavy_load, common = shares(count, rows * top, limit, slope, True), shares(count, rows * top, limit, slope, False)
    places = jnp.arange(count)

    def named(lengths, offset_by):
        used = int((lengths > 0).sum())
        fixed = max(1, used // 4)
        moved = fixed + (places - fixed + offset_by * (used - fixed)) % max(1, count - fixed)
        return jnp.zeros((count,), jnp.int32).at[ranking[jnp.where(places < fixed, places, moved)]].set(jnp.asarray(lengths, jnp.int32))

    lengths = jnp.where(number % 4 == 0, named(heavy_load, number // 4), named(common, number - number // 4 - 1))
    mixed = jax.random.permutation(jax.random.fold_in(own, 3), count)
    donor, sink = mixed[0:count // 2 * 2:2], mixed[1:count // 2 * 2:2]
    room = jnp.minimum(lengths[donor] - 1, limit - lengths[sink]) // 2
    room = jnp.where((donor == ranking[0]) | (sink == ranking[0]) | (lengths[sink] == 0), 0, jnp.maximum(room, 0))
    moved = jax.random.randint(jax.random.fold_in(own, 4), (count // 2,), 0, 1 << 20) % (room + 1)
    lengths = lengths.at[donor].add(-moved).at[sink].add(moved)
    items = jnp.searchsorted(jnp.cumsum(lengths), jnp.arange(rows * top), side="right").astype(jnp.int32)
    listing = items.reshape(top, rows).T
    listing = listing[jax.random.permutation(jax.random.fold_in(own, 1), rows)]
    offset_by = jax.random.randint(jax.random.fold_in(own, 2), (rows, 1), 0, top)
    return jnp.take_along_axis(listing, (jnp.arange(top)[None, :] + offset_by) % top, axis=1)


def shares(count, total, bound, slope, full):
    portions = [(1 << 20) // math.isqrt(rank ** slope) + 1 for rank in range(1, count + 1)]
    largest = bound if full else min(bound, max(-(-total // count), total * portions[0] // sum(portions)))
    least = 1 if total - largest >= count - 1 else 0
    holding, spare = [largest] + [least] * (count - 1), total - largest - least * (count - 1)
    while spare > 0:
        candidates = [i for i in range(1, count) if holding[i] < largest] or [i for i in range(1, count) if holding[i] < bound]
        pool, budget = sum([portions[i] for i in candidates]), spare
        for i in candidates:
            extra = min(bound - holding[i], max(1, budget * portions[i] // pool), spare)
            holding[i] = holding[i] + extra
            spare = spare - extra
    return np.array(holding)


def bell_draw(stream_key, dims, deviation, most, cuts=(), kind=jnp.bfloat16):
    values = jax.random.normal(stream_key, dims, jnp.float32) * deviation
    if len(cuts) > 0:
        values = steps_of(stream_key, dims, cuts, -0.22, 0.18) * values
    return jnp.clip(values, min=-most, max=most).astype(kind)


def setup_inputs(seed: int = 0) -> dict:
    arg_keys = jax.random.split(jax.random.key(seed), 8)
    tokens = bell_draw(arg_keys[0], (TOKENS, D), 1.0, 6.0, ((0, 32),))
    route_logits = bell_draw(arg_keys[1], (TOKENS, TOP), 1.5, 6.0, (), jnp.float32)
    expert_ids_keys = jax.random.split(jax.random.fold_in(arg_keys[2], 1), TOKENS // TOKENS)
    expert_ids_turns = jax.random.permutation(jax.random.fold_in(arg_keys[2], 3), TOKENS // TOKENS)
    expert_ids = jax.vmap(lambda own, number: assign_block(jax.random.fold_in(arg_keys[2], 2), own, number, TOKENS, EXPERTS, TOP, CAP, 2))(expert_ids_keys, expert_ids_turns).reshape((TOKENS, TOP))
    block_live = place_ends((jax.random.randint(arg_keys[3], (EXPERTS, FF // BLK), 0, 4) < 3).astype(jnp.int32), jax.random.fold_in(arg_keys[3], 1), 0, 1)
    w_gate = bell_draw(arg_keys[4], (EXPERTS, D, FF), D ** -0.5, 0.09375, ((0, 8), (2, 32)))
    w_up = bell_draw(arg_keys[5], (EXPERTS, D, FF), D ** -0.5, 0.09375, ((0, 8), (2, 32)))
    w_down = bell_draw(arg_keys[6], (EXPERTS, FF, D), FF ** -0.5, 0.046875, ((0, 8), (1, 32)))
    return dict(tokens=tokens, route_logits=route_logits, expert_ids=expert_ids, block_live=block_live, w_gate=w_gate, w_up=w_up, w_down=w_down)


def routing(expert_ids, route_logits, expert, capacity):
    chosen = (expert_ids == expert).astype(jnp.int32)
    flat_hits = chosen.reshape(-1)
    before = (jnp.cumsum(flat_hits) - flat_hits).reshape(chosen.shape)
    slot_pair = jnp.where(chosen > 0, before, capacity).astype(jnp.int32)
    leading = jax.nn.sigmoid(route_logits[:, 0] - route_logits[:, 1])
    mix_gates = jnp.stack([leading, 1.0 - leading], axis=1)
    weight = jnp.sum(mix_gates * chosen.astype(jnp.float32), axis=1)
    slot_tok = jnp.min(slot_pair, axis=1)
    slot_index = lax.broadcasted_iota(jnp.int32, (capacity, expert_ids.shape[0]), 0)
    dispatch = ((slot_pair[None, :, 0] == slot_index) | (slot_pair[None, :, 1] == slot_index)).astype(jnp.bfloat16)
    return dispatch, slot_tok, weight


def reference(tokens, route_logits, expert_ids, block_live, w_gate, w_up, w_down):
    capacity = CAP
    result = jnp.zeros((TOKENS, D), jnp.float32)
    for expert in range(EXPERTS):
        dispatch, slot_tok, weight = routing(expert_ids, route_logits, expert, capacity)
        gathered = jnp.dot(dispatch, tokens, preferred_element_type=jnp.float32).astype(jnp.bfloat16)
        gate_val = jnp.dot(gathered, w_gate[expert], preferred_element_type=jnp.float32)
        up_val = jnp.dot(gathered, w_up[expert], preferred_element_type=jnp.float32)
        live = jnp.repeat(block_live[expert].astype(jnp.float32), BLK)
        hidden = (jax.nn.silu(gate_val) * up_val * live[None, :]).astype(jnp.bfloat16)
        expert_out = jnp.dot(hidden, w_down[expert], preferred_element_type=jnp.float32)
        picked = jnp.take(expert_out, jnp.minimum(slot_tok, capacity - 1), axis=0)
        result = result + weight[:, None] * picked
    return result.astype(jnp.bfloat16)
```

```python
import jax
import jax.numpy as jnp
from jax import lax
from jax.sharding import PartitionSpec as P

BLK = 64


def routing(expert_ids, route_logits, expert, capacity):
    chosen = (expert_ids == expert).astype(jnp.int32)
    flat_hits = chosen.reshape(-1)
    before = (jnp.cumsum(flat_hits) - flat_hits).reshape(chosen.shape)
    slot_pair = jnp.where(chosen > 0, before, capacity)
    leading = jax.nn.sigmoid(route_logits[:, 0] - route_logits[:, 1])
    mix_gates = jnp.stack([leading, 1.0 - leading], axis=1)
    weight = jnp.sum(mix_gates * chosen.astype(jnp.float32), axis=1)
    slot_tok = jnp.min(slot_pair, axis=1)
    return slot_tok, weight


def per_device(planes, sites, tokens, route_logits, expert_ids, block_live, w_gate, w_up, w_down):
    total_tokens = expert_ids.shape[0]
    own_tokens, width = tokens.shape
    capacity = total_tokens // 2
    members = 2 * sites
    share = own_tokens // planes
    half = width // 2
    col = half // sites
    core = lax.axis_index("neuron") % 2
    partner = [(n, n ^ 1) for n in range(members)]
    same_core = [[2 * s + c for s in range(sites)] for c in range(2)]

    all_tokens = lax.all_gather(tokens, "neuron", axis=0, tiled=True)
    down = w_down[0]
    down_theirs = lax.dynamic_slice_in_dim(down, (1 - core) * half, half, axis=1)
    down_far = lax.ppermute(down_theirs, "neuron", partner)
    down_near = lax.dynamic_slice_in_dim(down, core * half, half, axis=1)

    slot_tok, weight = routing(expert_ids, route_logits, lax.axis_index("expert"), capacity)
    slot_index = lax.broadcasted_iota(jnp.int32, (capacity, total_tokens), 0)
    hit = slot_tok[None, :] == slot_index
    dispatch = hit.astype(jnp.bfloat16)
    slot_weight = jnp.sum(jnp.where(hit, weight[None, :], 0.0), axis=1)
    shuffled = slot_tok.reshape(members, planes, share).transpose(1, 0, 2).reshape(-1)
    spread = (
        shuffled[:, None] == lax.broadcasted_iota(jnp.int32, (total_tokens, capacity), 1)
    ).astype(jnp.bfloat16)

    gathered = jnp.dot(dispatch, all_tokens, preferred_element_type=jnp.float32).astype(jnp.bfloat16)
    gate_val = jnp.dot(gathered, w_gate[0], preferred_element_type=jnp.float32)
    up_val = jnp.dot(gathered, w_up[0], preferred_element_type=jnp.float32)
    live = jnp.repeat(block_live[0].astype(jnp.float32), BLK)
    hidden = (jax.nn.silu(gate_val) * up_val * live[None, :]).astype(jnp.bfloat16)
    hidden_far = lax.ppermute(hidden, "neuron", partner)
    partial = jnp.dot(hidden, down_near, preferred_element_type=jnp.float32) + jnp.dot(
        hidden_far, down_far, preferred_element_type=jnp.float32
    )
    partial = (partial * slot_weight[:, None]).astype(jnp.bfloat16)
    pieces = partial.reshape(capacity, sites, col).transpose(1, 0, 2)
    got = lax.all_to_all(pieces, "neuron", 0, 0, axis_index_groups=same_core, tiled=True)
    mine = jnp.sum(got.astype(jnp.float32), axis=0).astype(jnp.bfloat16)
    placed = jnp.dot(spread, mine, preferred_element_type=jnp.float32).astype(jnp.bfloat16)
    over = lax.all_to_all(placed.reshape(planes, members * share, col), "expert", 0, 0, tiled=True)
    mixed = jnp.sum(over.astype(jnp.float32), axis=0).astype(jnp.bfloat16)
    owned = lax.all_to_all(mixed.reshape(members, share, col), "neuron", 0, 0, tiled=True)
    copies = jnp.broadcast_to(owned.reshape(1, members * share, col), (planes, members * share, col))
    every = lax.all_to_all(copies, "expert", 0, 0, tiled=True)
    every = every.reshape(planes, sites, 2, share, col).transpose(0, 3, 2, 1, 4)
    return every.reshape(own_tokens, width)


def solution(mesh):
    placed = (
        P("neuron", None),
        P(),
        P(),
        P("expert", "neuron"),
        P("expert", None, "neuron"),
        P("expert", None, "neuron"),
        P("expert", "neuron", None),
    )

    def body(*args):
        return per_device(mesh.shape["expert"], mesh.shape["neuron"] // 2, *args)

    return jax.shard_map(
        body, mesh=mesh, in_specs=placed, out_specs=P("neuron", None), check_vma=False
    )
```

```python
import jax
import jax.numpy as jnp
from jax import lax
from jax.sharding import PartitionSpec as P

BLK = 64
RING = 4


def routing(expert_ids, route_logits, expert, capacity):
    chosen = (expert_ids == expert).astype(jnp.int32)
    flat_hits = chosen.reshape(-1)
    before = (jnp.cumsum(flat_hits) - flat_hits).reshape(chosen.shape)
    slot_pair = jnp.where(chosen > 0, before, capacity)
    leading = jax.nn.sigmoid(route_logits[:, 0] - route_logits[:, 1])
    mix_gates = jnp.stack([leading, 1.0 - leading], axis=1)
    weight = jnp.sum(mix_gates * chosen.astype(jnp.float32), axis=1)
    slot_tok = jnp.min(slot_pair, axis=1)
    return slot_tok, weight


def device(y, x, c):
    return ((y % RING) * RING + x % RING) * 2 + c


PLACES = [(y, x, c) for y in range(RING) for x in range(RING) for c in range(2)]
PARTNER = [(device(y, x, c), device(y, x, 1 - c)) for y, x, c in PLACES]
ALONG_X = [[device(y, x, c) for x in range(RING)] for y in range(RING) for c in range(2)]
ALONG_Y = [[device(y, x, c) for y in range(RING)] for x in range(RING) for c in range(2)]


def from_x(d):
    return [(device(y, x + d, c), device(y, x, c)) for y, x, c in PLACES]


def from_y(d):
    return [(device(y + d, x, c), device(y, x, c)) for y, x, c in PLACES]


def ring_gather(by_x, by_y):
    rows_x, rows_y = [by_x], [by_y]
    for d in (1, 3, 2):
        rows_x.append(lax.ppermute(by_x, "neuron", from_x(d)))
        rows_y.append(lax.ppermute(by_y, "neuron", from_y(d)))
    order = (0, 1, 3, 2)
    return [rows_x[k] for k in order], [rows_y[k] for k in order]


def per_device(planes, tokens, route_logits, expert_ids, block_live, w_gate, w_up, w_down):
    total_tokens = expert_ids.shape[0]
    own_tokens, width = tokens.shape
    capacity = total_tokens // 2
    sites = RING * RING
    members = 2 * sites
    share = own_tokens // planes
    half = width // 2
    col = half // sites
    place = lax.axis_index("neuron")
    core, x, y = place % 2, place // 2 % RING, place // (2 * RING)

    near = lax.dynamic_slice_in_dim(tokens, core * half, half, axis=1)
    far = lax.ppermute(
        lax.dynamic_slice_in_dim(tokens, (1 - core) * half, half, axis=1), "neuron", PARTNER
    )
    chip_rows = jnp.concatenate([near, far], axis=0)
    quarter = half // 2
    first_x, first_y = ring_gather(chip_rows[:, :quarter], chip_rows[:, quarter:])
    line_x, line_y = jnp.concatenate(first_x, axis=0), jnp.concatenate(first_y, axis=0)
    second_x, second_y = ring_gather(line_y, line_x)
    left, right = jnp.concatenate(second_y, axis=0), jnp.concatenate(second_x, axis=0)

    def halves(w, axis):
        return (
            lax.dynamic_slice_in_dim(w, core * half, half, axis=axis),
            lax.dynamic_slice_in_dim(w, (1 - core) * half, half, axis=axis),
        )

    down_near, down_theirs = halves(w_down[0], 1)
    down_far = lax.ppermute(down_theirs, "neuron", PARTNER)
    gate_near, gate_far = halves(w_gate[0], 0)
    up_near, up_far = halves(w_up[0], 0)

    slot_tok, weight = routing(expert_ids, route_logits, lax.axis_index("expert"), capacity)
    slot_index = lax.broadcasted_iota(jnp.int32, (capacity, total_tokens), 0)
    slot_weight = jnp.sum(jnp.where(slot_tok[None, :] == slot_index, weight[None, :], 0.0), axis=1)
    by_place = jnp.tile(slot_tok.reshape(RING, RING, 2, own_tokens), (2, 2, 2, 1))
    by_place = lax.dynamic_slice(by_place, (y, x, core, 0), (RING, RING, 2, own_tokens))
    pick_left = (by_place.reshape(1, -1) == slot_index).astype(jnp.bfloat16)
    pick_right = (by_place.transpose(1, 0, 2, 3).reshape(1, -1) == slot_index).astype(jnp.bfloat16)
    shuffled = slot_tok.reshape(members, planes, share).transpose(1, 0, 2).reshape(-1)
    spread = (
        shuffled[:, None] == lax.broadcasted_iota(jnp.int32, (total_tokens, capacity), 1)
    ).astype(jnp.bfloat16)

    def dot(a, b):
        return jnp.dot(a, b, preferred_element_type=jnp.float32)

    near_in = jnp.concatenate(
        [dot(pick_left, left).astype(jnp.bfloat16), dot(pick_right, right).astype(jnp.bfloat16)], axis=1
    )
    far_in = lax.ppermute(near_in, "neuron", PARTNER)
    gate_val = dot(near_in, gate_near) + dot(far_in, gate_far)
    up_val = dot(near_in, up_near) + dot(far_in, up_far)
    live = jnp.repeat(block_live[0].astype(jnp.float32), BLK)
    hidden = (jax.nn.silu(gate_val) * up_val * live[None, :]).astype(jnp.bfloat16)
    hidden_far = lax.ppermute(hidden, "neuron", PARTNER)
    partial = dot(hidden, down_near) + dot(hidden_far, down_far)
    partial = (partial * slot_weight[:, None]).astype(jnp.bfloat16)

    same_core = [[2 * s + c for s in range(sites)] for c in range(2)]
    pieces = partial.reshape(capacity, sites, col).transpose(1, 0, 2)
    got = lax.all_to_all(pieces, "neuron", 0, 0, axis_index_groups=same_core, tiled=True)
    mine = jnp.sum(got.astype(jnp.float32), axis=0).astype(jnp.bfloat16)
    placed = dot(spread, mine).astype(jnp.bfloat16)
    over = lax.all_to_all(placed.reshape(planes, members * share, col), "expert", 0, 0, tiled=True)
    mixed = jnp.sum(over.astype(jnp.float32), axis=0).astype(jnp.bfloat16)
    owned = lax.all_to_all(mixed.reshape(members, share, col), "neuron", 0, 0, tiled=True)
    copies = jnp.broadcast_to(owned.reshape(1, members * share, col), (planes, members * share, col))
    every = lax.all_to_all(copies, "expert", 0, 0, tiled=True)
    every = every.reshape(planes, sites, 2, share, col).transpose(0, 3, 2, 1, 4)
    return every.reshape(own_tokens, width)


def solution(mesh):
    placed = (
        P("neuron", None),
        P(),
        P(),
        P("expert", "neuron"),
        P("expert", None, "neuron"),
        P("expert", None, "neuron"),
        P("expert", "neuron", None),
    )

    def body(*args):
        return per_device(mesh.shape["expert"], *args)

    return jax.shard_map(
        body, mesh=mesh, in_specs=placed, out_specs=P("neuron", None), check_vma=False
    )
```

```python
import jax
import jax.numpy as jnp
from jax import lax
from jax.experimental import pallas as pl
from jax.experimental.pallas import tpu as pltpu
from jax.sharding import PartitionSpec as P


BLK = 64
RING = 4


def device(y, x, c):
    return ((y % RING) * RING + x % RING) * 2 + c


PLACES = [(y, x, c) for y in range(RING) for x in range(RING) for c in range(2)]
PARTNER = [(device(y, x, c), device(y, x, 1 - c)) for y, x, c in PLACES]


def from_x(d):
    return [(device(y, x + d, c), device(y, x, c)) for y, x, c in PLACES]


def from_y(d):
    return [(device(y + d, x, c), device(y, x, c)) for y, x, c in PLACES]


def to_x(d):
    return [(device(y, x, c), device(y, x + d, c)) for y, x, c in PLACES]


def to_y(d):
    return [(device(y, x, c), device(y + d, x, c)) for y, x, c in PLACES]


def ring_steps(by_x, by_y, perm_x, perm_y):
    got_x, got_y = {0: by_x[0]}, {0: by_y[0]}
    for d in STEPS:
        got_x[d] = lax.ppermute(by_x[d], "neuron", perm_x(d))
        got_y[d] = lax.ppermute(by_y[d], "neuron", perm_y(d))
    return [got_x[k] for k in range(RING)], [got_y[k] for k in range(RING)]


def ring_gather(by_x, by_y):
    return ring_steps([by_x] * RING, [by_y] * RING, from_x, from_y)


def ring_scatter(by_x, by_y):
    return ring_steps(by_x, by_y, to_x, to_y)


STEPS = (2, 1, 3)


def mm(a, b):
    return jnp.dot(a, b, preferred_element_type=jnp.float32)


def mm_t(a, b):
    return lax.dot_general(a, b, (((1,), (1,)), ((), ())), preferred_element_type=jnp.float32)


LIMIT = pltpu.CompilerParams(vmem_limit_bytes=20 * 2**20)


def whole(*arrays):
    return [pl.BlockSpec(a.shape, lambda i, s, n=len(a.shape): (0,) * n) for a in arrays]


def call(body, place, ins, specs, outs, scratch=(), flops=10**9, steps=1):
    return pl.pallas_call(
        body,
        grid_spec=pltpu.PrefetchScalarGridSpec(
            num_scalar_prefetch=1, grid=(steps,), in_specs=specs, out_specs=whole(*outs), scratch_shapes=list(scratch)
        ),
        out_shape=outs,
        compiler_params=LIMIT,
        cost_estimate=pl.CostEstimate(flops=flops, bytes_accessed=4 * 2**20, transcendentals=0),
    )(place, *ins)


def rows_kernel(place, mine, theirs, to_x_rows, to_y_rows):
    rows, span = mine.shape[0], to_x_rows.shape[1]
    for source, core in ((mine, place[0]), (theirs, 1 - place[0])):
        at = pl.ds(pl.multiple_of(core * rows, rows), rows)
        to_x_rows[at, :] = source[:, :span]
        to_y_rows[at, :] = source[:, span:]


def lines_kernel(place, *refs):
    for refs_in, out, start in ((refs[:RING], refs[-2], place[1]), (refs[RING:-2], refs[-1], place[2])):
        rows = refs_in[0].shape[0]
        for k in range(RING):
            out[pl.ds(pl.multiple_of((start + k) % RING * rows, rows), rows), :] = refs_in[k][...]


def routing_kernel(place, ids, logits, slots, slots_t, weight, spread):
    total_tokens, capacity = spread.shape
    lanes = 128
    first, second = (jnp.where(ids[k : k + 1, :] == place[3], 1.0, 0.0) for k in range(2))
    lead = 1.0 / (1.0 + jnp.exp(logits[1:2, :] - logits[0:1, :]))
    share = first * lead + second * (1.0 - lead)
    chosen = first + second
    chunks = [chosen[:, k : k + lanes] for k in range(0, total_tokens, lanes)]
    grid = jnp.concatenate(chunks, axis=0)
    earlier = lax.broadcasted_iota(jnp.int32, (lanes, lanes), 0) < lax.broadcasted_iota(jnp.int32, (lanes, lanes), 1)
    before = mm(grid.astype(jnp.bfloat16), jnp.where(earlier, 1.0, 0.0).astype(jnp.bfloat16))
    offset = jnp.zeros((1, 1), jnp.float32)
    out = []
    for k, chunk in enumerate(chunks):
        out.append(jnp.where(chunk > 0.0, before[k : k + 1, :] + offset, float(capacity)))
        offset = offset + jnp.sum(chunk, axis=1, keepdims=True)
    slot = jnp.concatenate(out, axis=1).astype(jnp.int32)
    slots[...] = slot
    per_chip = total_tokens // RING // RING
    slots_t[...] = jnp.concatenate(
        [slot[:, (y * RING + x) * per_chip : (y * RING + x + 1) * per_chip] for x in range(RING) for y in range(RING)], axis=1
    )
    hit = slot == lax.broadcasted_iota(jnp.int32, (capacity, total_tokens), 0)
    weight[...] = jnp.sum(jnp.where(hit, share, 0.0), axis=1, keepdims=True)
    planes, own = place_counts(total_tokens)
    each, part = own // planes, total_tokens // planes
    step = 256
    for top in range(0, total_tokens, step):
        row = lax.broadcasted_iota(jnp.int32, (step, total_tokens), 0) + top
        token = row % part // each * own + row // part * each + row % each
        column = lax.broadcasted_iota(jnp.int32, (step, total_tokens), 1)
        mine = jnp.sum(jnp.where(token == column, slot.astype(jnp.float32), 0.0), axis=1, keepdims=True)
        index = lax.broadcasted_iota(jnp.int32, (step, capacity), 1)
        spread[top : top + step, :] = jnp.where(mine.astype(jnp.int32) == index, 1.0, 0.0).astype(jnp.bfloat16)


def place_counts(total_tokens):
    return 8, total_tokens // len(PLACES)


def dispatch_kernel(place, slots, slots_t, *refs):
    blocks, out = refs[:-1], refs[-1]
    rows, span = blocks[0].shape
    capacity = out.shape[0]
    index = lax.broadcasted_iota(jnp.int32, (capacity, rows), 0)
    for side, (lines, start) in enumerate(((slots, place[2]), (slots_t, place[1]))):
        hot = []
        for k in range(RING):
            line = lines[:, pl.ds(pl.multiple_of((start + k) % RING * rows, rows), rows)]
            hot.append(jnp.where(line == index, 1.0, 0.0).astype(jnp.bfloat16))
        for n in range(0, span, 256):
            acc = mm(hot[0], blocks[side * RING][:, n : n + 256])
            for k in range(1, RING):
                acc = acc + mm(hot[k], blocks[side * RING + k][:, n : n + 256])
            out[:, side * span + n : side * span + n + 256] = acc.astype(jnp.bfloat16)


def near_kernel(place, rows, gate, up, gate_out, up_out):
    @pl.when(pl.program_id(0) == 0)
    def _():
        gate_out[...] = mm_t(rows[...], gate[...])
        up_out[...] = mm_t(rows[...], up[...])

    @pl.when(pl.program_id(0) > 0)
    def _():
        gate_out[...] += mm_t(rows[...], gate[...])
        up_out[...] += mm_t(rows[...], up[...])


def far_kernel(place, rows, gate, up, gate_near, up_near, live, out, gate_sum, up_sum):
    @pl.when(pl.program_id(0) == 0)
    def _():
        gate_sum[...] = gate_near[...] + mm_t(rows[...], gate[...])
        up_sum[...] = up_near[...] + mm_t(rows[...], up[...])

    @pl.when(pl.program_id(0) > 0)
    def _():
        gate_sum[...] += mm_t(rows[...], gate[...])
        up_sum[...] += mm_t(rows[...], up[...])

    @pl.when(pl.program_id(0) == pl.num_programs(0) - 1)
    def _():
        gate_val = gate_sum[...]
        block = lax.broadcasted_iota(jnp.int32, (1, out.shape[1]), 1) // BLK
        kept = jnp.zeros((1, out.shape[1]), jnp.float32)
        for k in range(out.shape[1] // BLK):
            kept = jnp.where(block == k, live[0, k].astype(jnp.float32), kept)
        out[...] = (gate_val / (1.0 + jnp.exp(-gate_val)) * up_sum[...] * kept).astype(jnp.bfloat16)


def down_kernel(place, near, far, w_near, w_far, weight, *refs):
    to_x_refs, to_y_refs, part = refs[:RING], refs[RING : 2 * RING], refs[-1]
    x, y = place[1], place[2]
    rows, span = to_x_refs[0].shape
    col = span // RING
    for e in range(RING):
        at = (y + e) % RING
        cols = pl.ds(pl.multiple_of(at * span, span), span)
        value = mm(near[...], w_near[:, cols]) + mm(far[...], w_far[:, cols])
        value = (value * weight[...]).astype(jnp.bfloat16)
        to_y_refs[e][...] = value[rows:]
        part[...] = value[:rows]
        for d in range(RING):
            block = part[:, pl.ds(pl.multiple_of((x + d) % RING * col, col), col)]
            to_x_refs[d][:, pl.ds(pl.multiple_of(at * col, col), col)] = block


def total(refs):
    value = refs[0][...].astype(jnp.float32)
    for r in refs[1:]:
        value = value + r[...].astype(jnp.float32)
    return value


def middle_kernel(place, *refs):
    got_x, got_y = refs[:RING], refs[RING : 2 * RING]
    to_y_refs, to_x_refs, part = refs[2 * RING : 3 * RING], refs[3 * RING : 4 * RING], refs[-1]
    col = to_y_refs[0].shape[1]
    for got, outs, start in ((got_x, to_y_refs, place[2]), (got_y, to_x_refs, place[1])):
        part[...] = total(got).astype(jnp.bfloat16)
        for k in range(RING):
            outs[k][...] = part[:, pl.ds(pl.multiple_of((start + k) % RING * col, col), col)]


def last_kernel(place, spread, *refs):
    got_y, got_x, out = refs[:RING], refs[RING : 2 * RING], refs[-1]
    rows = got_y[0].shape[0]
    value = mm(spread[:, :rows], total(got_y).astype(jnp.bfloat16))
    value = value + mm(spread[:, rows:], total(got_x).astype(jnp.bfloat16))
    out[...] = value.astype(jnp.bfloat16)


def per_device(planes, tokens, route_logits, expert_ids, block_live, w_gate, w_up, w_down):
    total_tokens = expert_ids.shape[0]
    own_tokens, width = tokens.shape
    capacity = total_tokens // 2
    sites = RING * RING
    members = 2 * sites
    share = own_tokens // planes
    half = width // 2
    col = half // sites
    place = lax.axis_index("neuron")
    core, x, y = place % 2, place // 2 % RING, place // (2 * RING)
    where = jnp.stack([core, x, y, lax.axis_index("expert")]).astype(jnp.int32)
    where, tokens = lax.optimization_barrier((where, tokens))
    shape = jax.ShapeDtypeStruct
    quarter = half // 2
    units = w_gate.shape[2]
    bf16 = jnp.bfloat16

    theirs = lax.ppermute(tokens, "neuron", PARTNER)
    own_half = pl.BlockSpec((own_tokens, half), lambda i, s: (0, s[0]))
    chip_rows = call(
        rows_kernel, where, (tokens, theirs), [own_half, own_half], [shape((2 * own_tokens, quarter), bf16)] * 2
    )
    *chip_rows, w_down, expert_ids, route_logits = lax.optimization_barrier((*chip_rows, w_down, expert_ids, route_logits))
    first_x, first_y = ring_gather(*chip_rows)
    down_far = lax.ppermute(w_down[0], "neuron", PARTNER)
    ins = (expert_ids.T, route_logits.T)
    routed = call(
        routing_kernel, where, ins, whole(*ins),
        [shape((1, total_tokens), jnp.int32)] * 2
        + [shape((capacity, 1), jnp.float32), shape((total_tokens, capacity), bf16)],
    )
    ins = (*first_x, *first_y)
    lines = call(lines_kernel, where, ins, whole(*ins), [shape((2 * RING * own_tokens, quarter), bf16)] * 2)
    line_x, line_y, *routed = lax.optimization_barrier((*lines, *routed))
    second_x, second_y = ring_gather(line_y, line_x)
    slots, slots_t, slot_weight, spread = routed

    ins = (slots, slots_t, *second_y, *second_x)
    near_in = call(
        dispatch_kernel, where, ins, whole(*ins), [shape((capacity, half), bf16)], flops=2 * capacity * total_tokens * half
    )[0]
    far_in = lax.ppermute(near_in, "neuron", PARTNER)
    gate, up = w_gate[0].T, w_up[0].T
    steps = 4
    cut = half // steps
    slab = pl.BlockSpec((capacity, cut), lambda i, s: (0, i))
    near_cut = pl.BlockSpec((units, cut), lambda i, s: (0, s[0] * steps + i))
    far_cut = pl.BlockSpec((units, cut), lambda i, s: (0, (1 - s[0]) * steps + i))
    down_half = pl.BlockSpec((units, half), lambda i, s: (0, s[0]))
    sums = call(
        near_kernel, where, (near_in, gate, up), [slab, near_cut, near_cut],
        [shape((capacity, units), jnp.float32)] * 2, flops=4 * capacity * half * units, steps=steps,
    )
    hidden = call(
        far_kernel, where, (far_in, gate, up, *sums, block_live), [slab, far_cut, far_cut, *whole(*sums), pl.BlockSpec(memory_space=pltpu.SMEM)],
        [shape((capacity, units), jnp.bfloat16)], [pltpu.VMEM((capacity, units), jnp.float32)] * 2,
        flops=4 * capacity * half * units, steps=steps,
    )[0]
    hidden_far = lax.ppermute(hidden, "neuron", PARTNER)
    rows = capacity // 2
    span = RING * col
    ins = (hidden, hidden_far, w_down[0], down_far, slot_weight)
    outs = call(
        down_kernel, where, ins,
        [*whole(hidden, hidden_far), down_half, down_half, *whole(slot_weight)],
        [shape((rows, span), jnp.bfloat16)] * (2 * RING), [pltpu.VMEM((rows, span), jnp.bfloat16)],
        flops=4 * capacity * half * units,
    )
    got_x, got_y = ring_scatter(outs[:RING], outs[RING:])
    ins = (*got_x, *got_y)
    outs = call(
        middle_kernel, where, ins, whole(*ins),
        [shape((rows, col), jnp.bfloat16)] * (2 * RING), [pltpu.VMEM((rows, span), jnp.bfloat16)],
    )
    got_x, got_y = ring_scatter(outs[RING:], outs[:RING])
    ins = (spread, *got_y, *got_x)
    placed = call(last_kernel, where, ins, whole(*ins), [shape((total_tokens, col), jnp.bfloat16)])[0]
    over = lax.all_to_all(placed.reshape(planes, members * share, col), "expert", 0, 0, tiled=True)
    mixed = jnp.sum(over.astype(jnp.float32), axis=0).astype(jnp.bfloat16)
    owned = lax.all_to_all(mixed.reshape(members, share, col), "neuron", 0, 0, tiled=True)
    copies = jnp.broadcast_to(owned.reshape(1, members * share, col), (planes, members * share, col))
    every = lax.all_to_all(copies, "expert", 0, 0, tiled=True)
    every = every.reshape(planes, sites, 2, share, col).transpose(0, 3, 2, 1, 4)
    return every.reshape(own_tokens, width)


def solution(mesh):
    placed = (
        P("neuron", None),
        P(),
        P(),
        P("expert", "neuron"),
        P("expert", None, "neuron"),
        P("expert", None, "neuron"),
        P("expert", "neuron", None),
    )

    def body(*args):
        return per_device(mesh.shape["expert"], *args)

    return jax.shard_map(body, mesh=mesh, in_specs=placed, out_specs=P("neuron", None), check_vma=False)
```

```python
import jax
import jax.numpy as jnp
from jax import lax
from jax.experimental import pallas as pl
from jax.experimental.pallas import tpu as pltpu
from jax.sharding import PartitionSpec as P


BLK = 64
RING = 4


def device(y, x, c):
    return ((y % RING) * RING + x % RING) * 2 + c


PLACES = [(y, x, c) for y in range(RING) for x in range(RING) for c in range(2)]
PARTNER = [(device(y, x, c), device(y, x, 1 - c)) for y, x, c in PLACES]


def turn(d, leg):
    pairs = []
    for y, x, c in PLACES:
        on = device(y, x + d, c) if c == leg else device(y + d, x, c)
        pairs.append((device(y, x, c), on))
    return pairs


def ring(leg, blocks, back):
    got = {0: blocks[0]}
    for d in STEPS:
        pairs = turn(d, leg)
        got[d] = lax.ppermute(blocks[d], "neuron", [(t, s) for s, t in pairs] if back else pairs)
    return [got[k] for k in range(RING)]


def relay(leg, left, right):
    on = turn(1, leg)
    back = [(t, s) for s, t in on]

    def send(value, pairs):
        return lax.ppermute(value, "neuron", pairs)

    left_before, right_after = send(left, on), send(right, back)
    right_before, left_after = send(right, on), send(left, back)
    left_far, right_far = send(left_before, on), send(right_after, back)
    return [left, left_after, left_far, left_before, right, right_after, right_far, right_before]


STEPS = (2, 1, 3)


def mm(a, b):
    return jnp.dot(a, b, preferred_element_type=jnp.float32)


LIMIT = pltpu.CompilerParams(vmem_limit_bytes=20 * 2**20)


def whole(*arrays):
    return [pl.BlockSpec(a.shape, lambda i, s, n=len(a.shape): (0,) * n) for a in arrays]


def call(body, place, ins, specs, outs, scratch=(), flops=10**9, steps=1):
    return pl.pallas_call(
        body,
        grid_spec=pltpu.PrefetchScalarGridSpec(
            num_scalar_prefetch=1, grid=(steps,), in_specs=specs, out_specs=whole(*outs), scratch_shapes=list(scratch)
        ),
        out_shape=outs,
        compiler_params=LIMIT,
        cost_estimate=pl.CostEstimate(flops=flops, bytes_accessed=4 * 2**20, transcendentals=0),
    )(place, *ins)


def rows_kernel(place, mine, theirs, out):
    rows = mine.shape[0]
    for source, core in ((mine, place[0]), (theirs, 1 - place[0])):
        out[pl.ds(pl.multiple_of(core * rows, rows), rows), :] = source[...]


def lines_kernel(place, *refs):
    rows, span = refs[0].shape[0], refs[-1].shape[1]
    for k in range(RING):
        at = pl.ds(pl.multiple_of((place[2] + k) % RING * rows, rows), rows)
        refs[-2][at, :] = refs[k][:, :span]
        refs[-1][at, :] = refs[k][:, span:]


def routing_kernel(place, ids, logits, slots, weight, spread):
    total_tokens, capacity = spread.shape
    lanes = 128
    first, second = (jnp.where(ids[k : k + 1, :] == place[1], 1.0, 0.0) for k in range(2))
    lead = 1.0 / (1.0 + jnp.exp(logits[1:2, :] - logits[0:1, :]))
    share = first * lead + second * (1.0 - lead)
    chosen = first + second
    chunks = [chosen[:, k : k + lanes] for k in range(0, total_tokens, lanes)]
    grid = jnp.concatenate(chunks, axis=0)
    earlier = lax.broadcasted_iota(jnp.int32, (lanes, lanes), 0) < lax.broadcasted_iota(jnp.int32, (lanes, lanes), 1)
    before = mm(grid.astype(jnp.bfloat16), jnp.where(earlier, 1.0, 0.0).astype(jnp.bfloat16))
    offset = jnp.zeros((1, 1), jnp.float32)
    out = []
    for k, chunk in enumerate(chunks):
        out.append(jnp.where(chunk > 0.0, before[k : k + 1, :] + offset, float(capacity)))
        offset = offset + jnp.sum(chunk, axis=1, keepdims=True)
    slot = jnp.concatenate(out, axis=1).astype(jnp.int32)
    per_chip = total_tokens // RING // RING
    across = jnp.concatenate(
        [slot[:, (y * RING + x) * per_chip : (y * RING + x + 1) * per_chip] for x in range(RING) for y in range(RING)], axis=1
    )
    slots[...] = jnp.where(place[0] == 0, slot, across)
    hit = slot == lax.broadcasted_iota(jnp.int32, (capacity, total_tokens), 0)
    weight[...] = jnp.sum(jnp.where(hit, share, 0.0), axis=1, keepdims=True)
    planes, own = place_counts(total_tokens)
    each, part = own // planes, total_tokens // planes
    step = 256
    for top in range(0, total_tokens, step):
        row = lax.broadcasted_iota(jnp.int32, (step, total_tokens), 0) + top
        token = row % part // each * own + row // part * each + row % each
        column = lax.broadcasted_iota(jnp.int32, (step, total_tokens), 1)
        mine = jnp.sum(jnp.where(token == column, slot.astype(jnp.float32), 0.0), axis=1, keepdims=True)
        index = lax.broadcasted_iota(jnp.int32, (step, capacity), 1)
        spread[top : top + step, :] = jnp.where(mine.astype(jnp.int32) == index, 1.0, 0.0).astype(jnp.bfloat16)


def place_counts(total_tokens):
    return 8, total_tokens // len(PLACES)


def dispatch_kernel(place, slots, *refs):
    blocks, out = refs[:-1], refs[-1]
    rows, span = blocks[0].shape
    capacity = out.shape[0]
    index = lax.broadcasted_iota(jnp.int32, (capacity, rows), 0)
    hot = []
    for k in range(RING):
        line = slots[:, pl.ds(pl.multiple_of((place[3] + k) % RING * rows, rows), rows)]
        hot.append(jnp.where(line == index, 1.0, 0.0).astype(jnp.bfloat16))
    for side in range(2):
        for n in range(0, span, 256):
            acc = mm(hot[0], blocks[side * RING][:, n : n + 256])
            for k in range(1, RING):
                acc = acc + mm(hot[k], blocks[side * RING + k][:, n : n + 256])
            out[:, side * span + n : side * span + n + 256] = acc.astype(jnp.bfloat16)


def turn_kernel(place, gate, up, out):
    units = gate.shape[0]
    out[:, :units] = gate[...].T
    out[:, units:] = up[...].T


def near_kernel(place, rows, both, out):
    out[...] = mm(rows[...], both[...])


def far_kernel(place, rows, both, near, live, keep, give, hidden):
    half_rows, units = keep.shape
    block = lax.broadcasted_iota(jnp.int32, (1, units), 1) // BLK
    kept = jnp.zeros((1, units), jnp.float32)
    for k in range(units // BLK):
        kept = jnp.where(block == k, live[0, k].astype(jnp.float32), kept)
    value = near[...] + mm(rows[...], both[...])
    gate_val, up_val = value[:, :units], value[:, units:]
    hidden[...] = (gate_val / (1.0 + jnp.exp(-gate_val)) * up_val * kept).astype(jnp.bfloat16)
    for out, core in ((keep, place[0]), (give, 1 - place[0])):
        out[...] = hidden[pl.ds(pl.multiple_of(core * half_rows, half_rows), half_rows), :]


def down_kernel(place, near, far, w_near, w_far, weight, *outs):
    rows, span = outs[0].shape
    col = span // RING
    scale = weight[pl.ds(pl.multiple_of(place[0] * rows, rows), rows), :]
    for d in range(RING):
        for j in range(RING):
            site = (place[2] + d) % RING * place[4] + j * place[5]
            cols = pl.ds(pl.multiple_of(site * col, col), col)
            value = mm(near[...], w_near[:, cols]) + mm(far[...], w_far[:, cols])
            outs[d][:, j * col : (j + 1) * col] = (value * scale).astype(jnp.bfloat16)


def total(refs):
    value = refs[0][...].astype(jnp.float32)
    for r in refs[1:]:
        value = value + r[...].astype(jnp.float32)
    return value


def middle_kernel(place, *refs):
    got, outs, part = refs[:RING], refs[RING : 2 * RING], refs[-1]
    col = outs[0].shape[1]
    part[...] = total(got).astype(jnp.bfloat16)
    for k in range(RING):
        outs[k][...] = part[:, pl.ds(pl.multiple_of((place[3] + k) % RING * col, col), col)]


def pair_kernel(place, *refs):
    got, outs, part = refs[:RING], refs[RING : RING + 2], refs[-1]
    col = outs[0].shape[1]
    part[...] = total(got).astype(jnp.bfloat16)
    for out, core in zip(outs, (place[0], 1 - place[0])):
        out[...] = part[:, pl.ds(pl.multiple_of(core * col, col), col)]


def last_kernel(place, spread, near, far, out):
    rows = near.shape[0]
    value = jnp.zeros(out.shape, jnp.float32)
    for part, core in ((near, place[0]), (far, 1 - place[0])):
        value = value + mm(spread[:, pl.ds(pl.multiple_of(core * rows, rows), rows)], part[...])
    out[...] = value.astype(jnp.bfloat16)


def per_device(planes, tokens, route_logits, expert_ids, block_live, w_gate, w_up, w_down):
    total_tokens = expert_ids.shape[0]
    own_tokens, width = tokens.shape
    capacity = total_tokens // 2
    sites = RING * RING
    members = 2 * sites
    share = own_tokens // planes
    half = width // 2
    col = half // sites
    place = lax.axis_index("neuron")
    core, x, y = place % 2, place // 2 % RING, place // (2 * RING)
    along_x = core == 0
    one, two = jnp.where(along_x, x, y), jnp.where(along_x, y, x)
    where = jnp.stack(
        [core, lax.axis_index("expert"), one, two, jnp.where(along_x, 1, RING), jnp.where(along_x, RING, 1)]
    ).astype(jnp.int32)
    where, tokens = lax.optimization_barrier((where, tokens))
    shape = jax.ShapeDtypeStruct
    units = w_gate.shape[2]
    bf16 = jnp.bfloat16

    theirs = lax.ppermute(tokens, "neuron", PARTNER)
    own_half = pl.BlockSpec((own_tokens, half), lambda i, s: (0, s[0]))
    chip_rows = call(rows_kernel, where, (tokens, theirs), [own_half, own_half], [shape((2 * own_tokens, half), bf16)])[0]
    chip_rows, w_down, expert_ids, route_logits = lax.optimization_barrier((chip_rows, w_down, expert_ids, route_logits))
    ins = ring(0, [chip_rows] * RING, True)
    down_far = lax.ppermute(w_down[0], "neuron", PARTNER)
    names = (expert_ids.T, route_logits.T)
    routed = call(
        routing_kernel, where, names, whole(*names),
        [shape((1, total_tokens), jnp.int32), shape((capacity, 1), jnp.float32), shape((total_tokens, capacity), bf16)],
    )
    line = call(lines_kernel, where, ins, whole(*ins), [shape((2 * RING * own_tokens, half // 2), bf16)] * 2)
    left, right, slots, slot_weight, spread = lax.optimization_barrier((*line, *routed))
    ins = (slots, *relay(1, left, right))
    cut = 512
    turned = pl.pallas_call(
        turn_kernel,
        grid_spec=pltpu.PrefetchScalarGridSpec(
            num_scalar_prefetch=1, grid=(width // cut,),
            in_specs=[pl.BlockSpec((units, cut), lambda i, s: (0, i))] * 2,
            out_specs=pl.BlockSpec((cut, 2 * units), lambda i, s: (i, 0)),
        ),
        out_shape=shape((width, 2 * units), bf16),
        compiler_params=LIMIT,
        cost_estimate=pl.CostEstimate(flops=10**9, bytes_accessed=4 * 2**20, transcendentals=0),
    )(where, w_gate[0].T, w_up[0].T)
    slots, turned = lax.optimization_barrier((ins[0], turned))
    ins = (slots, *ins[1:])
    near_in = call(
        dispatch_kernel, where, ins, whole(*ins), [shape((capacity, half), bf16)], flops=2 * capacity * total_tokens * half
    )[0]
    far_in = lax.ppermute(near_in, "neuron", PARTNER)
    near_half = pl.BlockSpec((half, 2 * units), lambda i, s: (s[0], 0))
    far_half = pl.BlockSpec((half, 2 * units), lambda i, s: (1 - s[0], 0))
    sums = call(
        near_kernel, where, (near_in, turned), [*whole(near_in), near_half],
        [shape((capacity, 2 * units), jnp.float32)], flops=4 * capacity * half * units,
    )
    rows = capacity // 2
    hidden, given = call(
        far_kernel, where, (far_in, turned, *sums, block_live),
        [*whole(far_in), far_half, *whole(*sums), pl.BlockSpec(memory_space=pltpu.SMEM)],
        [shape((rows, units), bf16)] * 2, [pltpu.VMEM((capacity, units), bf16)], flops=4 * capacity * half * units,
    )
    hidden_far = lax.ppermute(given, "neuron", PARTNER)
    ins = (hidden, hidden_far, w_down[0], down_far, slot_weight)
    pieces = call(
        down_kernel, where, ins, whole(*ins), [shape((rows, width // RING), bf16)] * RING, flops=4 * capacity * half * units
    )
    ins = ring(0, pieces, False)
    pieces = call(
        middle_kernel, where, ins, whole(*ins), [shape((rows, 2 * col), bf16)] * RING,
        [pltpu.VMEM((rows, width // RING), bf16)],
    )
    ins = ring(1, pieces, False)
    mine, given = call(
        pair_kernel, where, ins, whole(*ins), [shape((rows, col), bf16)] * 2, [pltpu.VMEM((rows, 2 * col), bf16)]
    )
    ins = (spread, mine, lax.ppermute(given, "neuron", PARTNER))
    placed = call(last_kernel, where, ins, whole(*ins), [shape((total_tokens, col), bf16)])[0]
    over = lax.all_to_all(placed.reshape(planes, members * share, col), "expert", 0, 0, tiled=True)
    mixed = jnp.sum(over.astype(jnp.float32), axis=0).astype(jnp.bfloat16)
    owned = lax.all_to_all(mixed.reshape(members, share, col), "neuron", 0, 0, tiled=True)
    copies = jnp.broadcast_to(owned.reshape(1, members * share, col), (planes, members * share, col))
    every = lax.all_to_all(copies, "expert", 0, 0, tiled=True)
    every = every.reshape(planes, members, share, col).transpose(0, 2, 1, 3)
    return every.reshape(own_tokens, width)


def solution(mesh):
    placed = (
        P("neuron", None),
        P(),
        P(),
        P("expert", "neuron"),
        P("expert", None, "neuron"),
        P("expert", None, "neuron"),
        P("expert", "neuron", None),
    )

    def body(*args):
        return per_device(mesh.shape["expert"], *args)

    return jax.shard_map(body, mesh=mesh, in_specs=placed, out_specs=P("neuron", None), check_vma=False)
```

```python
import functools

import jax
import jax.numpy as jnp
from jax import lax
from jax.experimental import pallas as pl
from jax.experimental.pallas import tpu as pltpu
from jax.sharding import PartitionSpec as P


BLK = 64
RING = 4


def device(y, x, c):
    return ((y % RING) * RING + x % RING) * 2 + c


PLACES = [(y, x, c) for y in range(RING) for x in range(RING) for c in range(2)]
PARTNER = [(device(y, x, c), device(y, x, 1 - c)) for y, x, c in PLACES]


def turn(d, leg):
    pairs = []
    for y, x, c in PLACES:
        on = device(y, x + d, c) if c == leg else device(y + d, x, c)
        pairs.append((device(y, x, c), on))
    return pairs


def ring(leg, blocks, back):
    got = {0: blocks[0]}
    for d in STEPS:
        pairs = turn(d, leg)
        got[d] = lax.ppermute(blocks[d], "neuron", [(t, s) for s, t in pairs] if back else pairs)
    return [got[k] for k in range(RING)]


def relay(leg, left, right):
    on = turn(1, leg)
    back = [(t, s) for s, t in on]

    def send(value, pairs):
        return lax.ppermute(value, "neuron", pairs)

    left_before, right_after = send(left, on), send(right, back)
    right_before, left_after = send(right, on), send(left, back)
    left_far, right_far = send(left_before, on), send(right_after, back)
    return [left, left_after, left_before, right, right_after, right_before], left_far, right_far


STEPS = (2, 1, 3)
DOWN_STEPS = ((2,), (1, 3), (0,))


def mm(a, b):
    return jnp.dot(a, b, preferred_element_type=jnp.float32)


LIMIT = pltpu.CompilerParams(vmem_limit_bytes=20 * 2**20)


def whole(*arrays):
    return [pl.BlockSpec(a.shape, lambda i, s, n=len(a.shape): (0,) * n) for a in arrays]


def call(body, place, ins, specs, outs, scratch=(), flops=10**9, steps=1):
    return pl.pallas_call(
        body,
        grid_spec=pltpu.PrefetchScalarGridSpec(
            num_scalar_prefetch=1, grid=(steps,), in_specs=specs, out_specs=whole(*outs), scratch_shapes=list(scratch)
        ),
        out_shape=outs,
        compiler_params=LIMIT,
        cost_estimate=pl.CostEstimate(flops=flops, bytes_accessed=4 * 2**20, transcendentals=0),
    )(place, *ins)


def rows_kernel(place, mine, theirs, out):
    rows = mine.shape[0]
    for source, core in ((mine, place[0]), (theirs, 1 - place[0])):
        out[pl.ds(pl.multiple_of(core * rows, rows), rows), :] = source[...]


def lines_kernel(place, *refs):
    rows, span = refs[0].shape[0], refs[-1].shape[1]
    for k in range(RING):
        at = pl.ds(pl.multiple_of((place[2] + k) % RING * rows, rows), rows)
        refs[-2][at, :] = refs[k][:, :span]
        refs[-1][at, :] = refs[k][:, span:]


def routing_kernel(place, ids, logits, slots, weight, spread):
    total_tokens, capacity = spread.shape
    lanes = 128
    first, second = (jnp.where(ids[k : k + 1, :] == place[1], 1.0, 0.0) for k in range(2))
    lead = 1.0 / (1.0 + jnp.exp(logits[1:2, :] - logits[0:1, :]))
    share = first * lead + second * (1.0 - lead)
    chosen = first + second
    chunks = [chosen[:, k : k + lanes] for k in range(0, total_tokens, lanes)]
    grid = jnp.concatenate(chunks, axis=0)
    earlier = lax.broadcasted_iota(jnp.int32, (lanes, lanes), 0) < lax.broadcasted_iota(jnp.int32, (lanes, lanes), 1)
    before = mm(grid.astype(jnp.bfloat16), jnp.where(earlier, 1.0, 0.0).astype(jnp.bfloat16))
    offset = jnp.zeros((1, 1), jnp.float32)
    out = []
    for k, chunk in enumerate(chunks):
        out.append(jnp.where(chunk > 0.0, before[k : k + 1, :] + offset, float(capacity)))
        offset = offset + jnp.sum(chunk, axis=1, keepdims=True)
    slot = jnp.concatenate(out, axis=1).astype(jnp.int32)
    per_chip = total_tokens // RING // RING
    across = jnp.concatenate(
        [slot[:, (y * RING + x) * per_chip : (y * RING + x + 1) * per_chip] for x in range(RING) for y in range(RING)], axis=1
    )
    slots[...] = jnp.where(place[0] == 0, slot, across)
    hit = slot == lax.broadcasted_iota(jnp.int32, (capacity, total_tokens), 0)
    weight[...] = jnp.sum(jnp.where(hit, share, 0.0), axis=1, keepdims=True)
    planes, own = place_counts(total_tokens)
    each, part = own // planes, total_tokens // planes
    step = 256
    for top in range(0, total_tokens, step):
        row = lax.broadcasted_iota(jnp.int32, (step, total_tokens), 0) + top
        token = row % part // each * own + row // part * each + row % each
        column = lax.broadcasted_iota(jnp.int32, (step, total_tokens), 1)
        mine = jnp.sum(jnp.where(token == column, slot.astype(jnp.float32), 0.0), axis=1, keepdims=True)
        index = lax.broadcasted_iota(jnp.int32, (step, capacity), 1)
        spread[top : top + step, :] = jnp.where(mine.astype(jnp.int32) == index, 1.0, 0.0).astype(jnp.bfloat16)


def place_counts(total_tokens):
    return 8, total_tokens // len(PLACES)


def hot_rows(place, slots, k, capacity, rows):
    line = slots[:, pl.ds(pl.multiple_of((place[3] + k) % RING * rows, rows), rows)]
    index = lax.broadcasted_iota(jnp.int32, (capacity, rows), 0)
    return jnp.where(line == index, 1.0, 0.0).astype(jnp.bfloat16)


def dispatch_kernel(place, slots, *refs):
    outs = refs[-2:]
    rows, span = refs[0].shape
    hot = [hot_rows(place, slots, k, outs[0].shape[0], rows) for k in (0, 1, 3)]
    for side, out in enumerate(outs):
        blocks = refs[3 * side : 3 * side + 3]
        for n in range(0, span, 256):
            acc = mm(hot[0], blocks[0][:, n : n + 256])
            acc = acc + mm(hot[1], blocks[1][:, n : n + 256]) + mm(hot[2], blocks[2][:, n : n + 256])
            out[:, n : n + 256] = acc.astype(jnp.bfloat16)


def finish_kernel(place, slots, part, block, out):
    rows, span = block.shape
    hot = hot_rows(place, slots, 2, out.shape[0], rows)
    for n in range(0, span, 256):
        acc = part[:, n : n + 256].astype(jnp.float32) + mm(hot, block[:, n : n + 256])
        out[:, n : n + 256] = acc.astype(jnp.bfloat16)


def turn_kernel(place, gate, up, out):
    units = gate.shape[0]
    out[:, :units] = gate[...].T
    out[:, units:] = up[...].T


def near_kernel(place, left, right, both, out):
    cut = left.shape[1]
    out[...] = mm(left[...], both[:cut, :]) + mm(right[...], both[cut:, :])


def far_kernel(place, left, right, both, near, live, out):
    cut, units = left.shape[1], out.shape[1]
    block = lax.broadcasted_iota(jnp.int32, (1, units), 1) // BLK
    kept = jnp.zeros((1, units), jnp.float32)
    for k in range(units // BLK):
        kept = jnp.where(block == k, live[0, k].astype(jnp.float32), kept)
    value = near[...] + (mm(left[...], both[:cut, :]) + mm(right[...], both[cut:, :]))
    gate_val, up_val = value[:, :units], value[:, units:]
    out[...] = (gate_val / (1.0 + jnp.exp(-gate_val)) * up_val * kept).astype(jnp.bfloat16)


def down_kernel(steps, place, near, far, w_near, w_far, weight, *outs):
    rows, span = outs[0].shape
    col = span // RING
    scale = weight[pl.ds(pl.multiple_of(place[0] * rows, rows), rows), :]
    for d, out in zip(steps, outs):
        for j in range(RING):
            site = (place[2] + d) % RING * place[4] + j * place[5]
            cols = pl.ds(pl.multiple_of(site * col, col), col)
            value = mm(near[...], w_near[:, cols]) + mm(far[...], w_far[:, cols])
            out[:, j * col : (j + 1) * col] = (value * scale).astype(jnp.bfloat16)


def total(refs):
    value = refs[0][...].astype(jnp.float32)
    for r in refs[1:]:
        value = value + r[...].astype(jnp.float32)
    return value


def middle_kernel(place, *refs):
    got, outs, part = refs[:RING], refs[RING : 2 * RING], refs[-1]
    col = outs[0].shape[1]
    part[...] = total(got).astype(jnp.bfloat16)
    for k in range(RING):
        outs[k][...] = part[:, pl.ds(pl.multiple_of((place[3] + k) % RING * col, col), col)]


def pair_kernel(place, *refs):
    got, outs, part = refs[:RING], refs[RING : RING + 2], refs[-1]
    col = outs[0].shape[1]
    part[...] = total(got).astype(jnp.bfloat16)
    for out, core in zip(outs, (place[0], 1 - place[0])):
        out[...] = part[:, pl.ds(pl.multiple_of(core * col, col), col)]


def last_kernel(place, spread, near, far, out):
    rows = near.shape[0]
    value = jnp.zeros(out.shape, jnp.float32)
    for part, core in ((near, place[0]), (far, 1 - place[0])):
        value = value + mm(spread[:, pl.ds(pl.multiple_of(core * rows, rows), rows)], part[...])
    out[...] = value.astype(jnp.bfloat16)


def per_device(planes, tokens, route_logits, expert_ids, block_live, w_gate, w_up, w_down):
    total_tokens = expert_ids.shape[0]
    own_tokens, width = tokens.shape
    capacity = total_tokens // 2
    sites = RING * RING
    members = 2 * sites
    share = own_tokens // planes
    half = width // 2
    col = half // sites
    place = lax.axis_index("neuron")
    core, x, y = place % 2, place // 2 % RING, place // (2 * RING)
    along_x = core == 0
    one, two = jnp.where(along_x, x, y), jnp.where(along_x, y, x)
    where = jnp.stack(
        [core, lax.axis_index("expert"), one, two, jnp.where(along_x, 1, RING), jnp.where(along_x, RING, 1)]
    ).astype(jnp.int32)
    where, tokens = lax.optimization_barrier((where, tokens))
    shape = jax.ShapeDtypeStruct
    units = w_gate.shape[2]
    bf16 = jnp.bfloat16

    theirs = lax.ppermute(tokens, "neuron", PARTNER)
    own_half = pl.BlockSpec((own_tokens, half), lambda i, s: (0, s[0]))
    chip_rows = call(rows_kernel, where, (tokens, theirs), [own_half, own_half], [shape((2 * own_tokens, half), bf16)])[0]
    chip_rows, w_down, expert_ids, route_logits = lax.optimization_barrier((chip_rows, w_down, expert_ids, route_logits))
    ins = ring(0, [chip_rows] * RING, True)
    down_far = lax.ppermute(w_down[0], "neuron", PARTNER)
    names = (expert_ids.T, route_logits.T)
    routed = call(
        routing_kernel, where, names, whole(*names),
        [shape((1, total_tokens), jnp.int32), shape((capacity, 1), jnp.float32), shape((total_tokens, capacity), bf16)],
    )
    line = call(lines_kernel, where, ins, whole(*ins), [shape((2 * RING * own_tokens, half // 2), bf16)] * 2)
    left, right, slots, slot_weight, spread = lax.optimization_barrier((*line, *routed))
    cut = 512
    turned = pl.pallas_call(
        turn_kernel,
        grid_spec=pltpu.PrefetchScalarGridSpec(
            num_scalar_prefetch=1, grid=(width // cut,),
            in_specs=[pl.BlockSpec((units, cut), lambda i, s: (0, i))] * 2,
            out_specs=pl.BlockSpec((cut, 2 * units), lambda i, s: (i, 0)),
        ),
        out_shape=shape((width, 2 * units), bf16),
        compiler_params=LIMIT,
        cost_estimate=pl.CostEstimate(flops=10**9, bytes_accessed=4 * 2**20, transcendentals=0),
    )(where, w_gate[0].T, w_up[0].T)
    blocks, left_far, right_far = relay(1, left, right)
    slots, turned = lax.optimization_barrier((slots, turned))
    ins = (slots, *blocks)
    parts = call(
        dispatch_kernel, where, ins, whole(*ins), [shape((capacity, half // 2), bf16)] * 2, flops=capacity * total_tokens * half
    )
    near_in, far_in = [], []
    for part, block in ((parts[0], left_far), (parts[1], right_far)):
        ins = (slots, part, block)
        near_in += call(finish_kernel, where, ins, whole(*ins), [shape((capacity, half // 2), bf16)], flops=capacity**2 * half)
        far_in.append(lax.ppermute(near_in[-1], "neuron", PARTNER))
    near_half = pl.BlockSpec((half, 2 * units), lambda i, s: (s[0], 0))
    far_half = pl.BlockSpec((half, 2 * units), lambda i, s: (1 - s[0], 0))
    sums = call(
        near_kernel, where, (*near_in, turned), [*whole(*near_in), near_half],
        [shape((capacity, 2 * units), jnp.float32)], flops=4 * capacity * half * units,
    )[0]
    rows = capacity // 2

    def far_rows(which):
        def half_of(span):
            return pl.BlockSpec((rows, span), lambda i, s: (which(s[0]), 0))

        return call(
            far_kernel, where, (*far_in, turned, sums, block_live),
            [half_of(half // 2), half_of(half // 2), far_half, half_of(2 * units), pl.BlockSpec(memory_space=pltpu.SMEM)],
            [shape((rows, units), bf16)], flops=2 * capacity * half * units,
        )[0]

    given = far_rows(lambda c: 1 - c)
    hidden_far = lax.ppermute(given, "neuron", PARTNER)
    hidden = far_rows(lambda c: c)
    ins = (hidden, hidden_far, w_down[0], down_far, slot_weight)
    pieces = {}
    for steps in DOWN_STEPS:
        outs = call(
            functools.partial(down_kernel, steps), where, ins, whole(*ins),
            [shape((rows, width // RING), bf16)] * len(steps), flops=len(steps) * capacity * half * units,
        )
        pieces.update(zip(steps, outs))
    ins = ring(0, pieces, False)
    pieces = call(
        middle_kernel, where, ins, whole(*ins), [shape((rows, 2 * col), bf16)] * RING,
        [pltpu.VMEM((rows, width // RING), bf16)],
    )
    ins = ring(1, pieces, False)
    mine, given = call(
        pair_kernel, where, ins, whole(*ins), [shape((rows, col), bf16)] * 2, [pltpu.VMEM((rows, 2 * col), bf16)]
    )
    ins = (spread, mine, lax.ppermute(given, "neuron", PARTNER))
    placed = call(last_kernel, where, ins, whole(*ins), [shape((total_tokens, col), bf16)])[0]
    over = lax.all_to_all(placed.reshape(planes, members * share, col), "expert", 0, 0, tiled=True)
    mixed = jnp.sum(over.astype(jnp.float32), axis=0).astype(jnp.bfloat16)
    owned = lax.all_to_all(mixed.reshape(members, share, col), "neuron", 0, 0, tiled=True)
    copies = jnp.broadcast_to(owned.reshape(1, members * share, col), (planes, members * share, col))
    every = lax.all_to_all(copies, "expert", 0, 0, tiled=True)
    every = every.reshape(planes, members, share, col).transpose(0, 2, 1, 3)
    return every.reshape(own_tokens, width)


def solution(mesh):
    placed = (
        P("neuron", None),
        P(),
        P(),
        P("expert", "neuron"),
        P("expert", None, "neuron"),
        P("expert", None, "neuron"),
        P("expert", "neuron", None),
    )

    def body(*args):
        return per_device(mesh.shape["expert"], *args)

    return jax.shard_map(body, mesh=mesh, in_specs=placed, out_specs=P("neuron", None), check_vma=False)
```

```python
import functools

import jax
import jax.numpy as jnp
from jax import lax
from jax.experimental import pallas as pl
from jax.experimental.pallas import tpu as pltpu
from jax.sharding import PartitionSpec as P


BLK = 64
RING = 4


def device(y, x, c):
    return ((y % RING) * RING + x % RING) * 2 + c


PLACES = [(y, x, c) for y in range(RING) for x in range(RING) for c in range(2)]
PARTNER = [(device(y, x, c), device(y, x, 1 - c)) for y, x, c in PLACES]


def turn(d, leg):
    pairs = []
    for y, x, c in PLACES:
        on = device(y, x + d, c) if c == leg else device(y + d, x, c)
        pairs.append((device(y, x, c), on))
    return pairs


def ring(leg, blocks, back):
    got = {0: blocks[0]}
    for d in STEPS:
        pairs = turn(d, leg)
        got[d] = lax.ppermute(blocks[d], "neuron", [(t, s) for s, t in pairs] if back else pairs)
    return [got[k] for k in range(RING)]


def relay(leg, left, right):
    on = turn(1, leg)
    back = [(t, s) for s, t in on]

    def send(value, pairs):
        return lax.ppermute(value, "neuron", pairs)

    left_before, right_after = send(left, on), send(right, back)
    right_before, left_after = send(right, on), send(left, back)
    left_far, right_far = send(left_before, on), send(right_after, back)
    return [left, left_after, left_before, right, right_after, right_before], left_far, right_far


STEPS = (2, 1, 3)
DOWN_STEPS = ((2,), (1, 3), (0,))


def mm(a, b):
    return jnp.dot(a, b, preferred_element_type=jnp.float32)


LIMIT = pltpu.CompilerParams(vmem_limit_bytes=20 * 2**20)


def whole(*arrays):
    return [pl.BlockSpec(a.shape, lambda i, s, n=len(a.shape): (0,) * n) for a in arrays]


def call(body, place, ins, specs, outs, scratch=(), flops=10**9, steps=1):
    return pl.pallas_call(
        body,
        grid_spec=pltpu.PrefetchScalarGridSpec(
            num_scalar_prefetch=1, grid=(steps,), in_specs=specs, out_specs=whole(*outs), scratch_shapes=list(scratch)
        ),
        out_shape=outs,
        compiler_params=LIMIT,
        cost_estimate=pl.CostEstimate(flops=flops, bytes_accessed=4 * 2**20, transcendentals=0),
    )(place, *ins)


def rows_kernel(place, mine, theirs, out):
    rows = mine.shape[0]
    for source, core in ((mine, place[0]), (theirs, 1 - place[0])):
        out[pl.ds(pl.multiple_of(core * rows, rows), rows), :] = source[...]


def copy_kernel(place, source, out):
    out[...] = source[...]


def lines_kernel(place, *refs):
    rows, span = refs[0].shape[0], refs[-1].shape[1]
    for k in range(RING):
        at = pl.ds(pl.multiple_of((place[2] + k) % RING * rows, rows), rows)
        refs[-2][at, :] = refs[k][:, :span]
        refs[-1][at, :] = refs[k][:, span:]


def routing_kernel(place, ids, logits, slots, weight, spread):
    total_tokens, capacity = spread.shape
    lanes = 128
    first, second = (jnp.where(ids[k : k + 1, :] == place[1], 1.0, 0.0) for k in range(2))
    lead = 1.0 / (1.0 + jnp.exp(logits[1:2, :] - logits[0:1, :]))
    share = first * lead + second * (1.0 - lead)
    chosen = first + second
    chunks = [chosen[:, k : k + lanes] for k in range(0, total_tokens, lanes)]
    grid = jnp.concatenate(chunks, axis=0)
    earlier = lax.broadcasted_iota(jnp.int32, (lanes, lanes), 0) < lax.broadcasted_iota(jnp.int32, (lanes, lanes), 1)
    before = mm(grid.astype(jnp.bfloat16), jnp.where(earlier, 1.0, 0.0).astype(jnp.bfloat16))
    offset = jnp.zeros((1, 1), jnp.float32)
    out = []
    for k, chunk in enumerate(chunks):
        out.append(jnp.where(chunk > 0.0, before[k : k + 1, :] + offset, float(capacity)))
        offset = offset + jnp.sum(chunk, axis=1, keepdims=True)
    slot = jnp.concatenate(out, axis=1).astype(jnp.int32)
    per_chip = total_tokens // RING // RING
    across = jnp.concatenate(
        [slot[:, (y * RING + x) * per_chip : (y * RING + x + 1) * per_chip] for x in range(RING) for y in range(RING)], axis=1
    )
    slots[...] = jnp.where(place[0] == 0, slot, across)
    hit = slot == lax.broadcasted_iota(jnp.int32, (capacity, total_tokens), 0)
    weight[...] = jnp.sum(jnp.where(hit, share, 0.0), axis=1, keepdims=True)
    planes, own = place_counts(total_tokens)
    each, part = own // planes, total_tokens // planes
    step = 256
    for top in range(0, total_tokens, step):
        row = lax.broadcasted_iota(jnp.int32, (step, total_tokens), 0) + top
        token = row % part // each * own + row // part * each + row % each
        column = lax.broadcasted_iota(jnp.int32, (step, total_tokens), 1)
        mine = jnp.sum(jnp.where(token == column, slot.astype(jnp.float32), 0.0), axis=1, keepdims=True)
        index = lax.broadcasted_iota(jnp.int32, (step, capacity), 1)
        spread[top : top + step, :] = jnp.where(mine.astype(jnp.int32) == index, 1.0, 0.0).astype(jnp.bfloat16)


def place_counts(total_tokens):
    return 8, total_tokens // len(PLACES)


def hot_rows(place, slots, k, capacity, rows):
    line = slots[:, pl.ds(pl.multiple_of((place[3] + k) % RING * rows, rows), rows)]
    index = lax.broadcasted_iota(jnp.int32, (capacity, rows), 0)
    return jnp.where(line == index, 1.0, 0.0).astype(jnp.bfloat16)


def dispatch_kernel(place, slots, *refs):
    outs = refs[-2:]
    rows, span = refs[0].shape
    hot = [hot_rows(place, slots, k, outs[0].shape[0], rows) for k in (0, 1, 3)]
    for side, out in enumerate(outs):
        blocks = refs[3 * side : 3 * side + 3]
        for n in range(0, span, 256):
            acc = mm(hot[0], blocks[0][:, n : n + 256])
            acc = acc + mm(hot[1], blocks[1][:, n : n + 256]) + mm(hot[2], blocks[2][:, n : n + 256])
            out[:, n : n + 256] = acc.astype(jnp.bfloat16)


def finish_kernel(place, slots, part, block, out):
    rows, span = block.shape
    hot = hot_rows(place, slots, 2, out.shape[0], rows)
    for n in range(0, span, 256):
        acc = part[:, n : n + 256].astype(jnp.float32) + mm(hot, block[:, n : n + 256])
        out[:, n : n + 256] = acc.astype(jnp.bfloat16)


def turn_kernel(place, gate, up, out):
    units = gate.shape[0]
    out[:, :units] = gate[...].T
    out[:, units:] = up[...].T


def near_kernel(place, left, right, both, out):
    cut = left.shape[1]
    out[...] = mm(left[...], both[:cut, :]) + mm(right[...], both[cut:, :])


def far_kernel(place, left, right, both, near, live, out):
    cut, units = left.shape[1], out.shape[1]
    block = lax.broadcasted_iota(jnp.int32, (1, units), 1) // BLK
    kept = jnp.zeros((1, units), jnp.float32)
    for k in range(units // BLK):
        kept = jnp.where(block == k, live[0, k].astype(jnp.float32), kept)
    value = near[...] + (mm(left[...], both[:cut, :]) + mm(right[...], both[cut:, :]))
    gate_val, up_val = value[:, :units], value[:, units:]
    out[...] = (gate_val / (1.0 + jnp.exp(-gate_val)) * up_val * kept).astype(jnp.bfloat16)


def down_kernel(steps, place, near, far, w_near, w_far, weight, *outs):
    rows, span = outs[0].shape
    col = span // RING
    scale = weight[pl.ds(pl.multiple_of(place[0] * rows, rows), rows), :]
    for d, out in zip(steps, outs):
        for j in range(RING):
            site = (place[2] + d) % RING * place[4] + j * place[5]
            cols = pl.ds(pl.multiple_of(site * col, col), col)
            value = mm(near[...], w_near[:, cols]) + mm(far[...], w_far[:, cols])
            out[:, j * col : (j + 1) * col] = (value * scale).astype(jnp.bfloat16)


def total_of(refs, block, col):
    cols = pl.ds(pl.multiple_of(block * col, col), col)
    value = refs[0][:, cols].astype(jnp.float32)
    for r in refs[1:]:
        value = value + r[:, cols].astype(jnp.float32)
    return value.astype(jnp.bfloat16)


def middle_kernel(steps, place, *refs):
    got, outs = refs[:RING], refs[RING:]
    for k, out in zip(steps, outs):
        out[...] = total_of(got, (place[3] + k) % RING, out.shape[1])


def given_kernel(place, *refs):
    refs[-1][...] = total_of(refs[:-1], 1 - place[0], refs[-1].shape[1])


def placed_kernel(place, spread, *refs):
    got, out = refs[:-1], refs[-1]
    rows = got[0].shape[0]
    at = pl.ds(pl.multiple_of(place[0] * rows, rows), rows)
    out[...] = mm(spread[:, at], total_of(got, place[0], out.shape[1]))


def last_kernel(place, spread, near, far, out):
    rows = far.shape[0]
    at = pl.ds(pl.multiple_of((1 - place[0]) * rows, rows), rows)
    out[...] = (near[...] + mm(spread[:, at], far[...])).astype(jnp.bfloat16)


def per_device(planes, tokens, route_logits, expert_ids, block_live, w_gate, w_up, w_down):
    total_tokens = expert_ids.shape[0]
    own_tokens, width = tokens.shape
    capacity = total_tokens // 2
    sites = RING * RING
    members = 2 * sites
    share = own_tokens // planes
    half = width // 2
    col = half // sites
    place = lax.axis_index("neuron")
    core, x, y = place % 2, place // 2 % RING, place // (2 * RING)
    along_x = core == 0
    one, two = jnp.where(along_x, x, y), jnp.where(along_x, y, x)
    where = jnp.stack(
        [core, lax.axis_index("expert"), one, two, jnp.where(along_x, 1, RING), jnp.where(along_x, RING, 1)]
    ).astype(jnp.int32)
    where, tokens = lax.optimization_barrier((where, tokens))
    shape = jax.ShapeDtypeStruct
    units = w_gate.shape[2]
    bf16 = jnp.bfloat16

    theirs = lax.ppermute(tokens, "neuron", PARTNER)
    own_half = pl.BlockSpec((own_tokens, half), lambda i, s: (0, s[0]))
    mine = call(copy_kernel, where, (tokens,), [own_half], [shape((own_tokens, half), bf16)])[0]
    chip_rows = call(
        rows_kernel, where, (mine, theirs), [*whole(mine), own_half], [shape((2 * own_tokens, half), bf16)]
    )[0]
    chip_rows, w_down, expert_ids, route_logits = lax.optimization_barrier((chip_rows, w_down, expert_ids, route_logits))
    ins = ring(0, [chip_rows] * RING, True)
    down_far = lax.ppermute(w_down[0], "neuron", PARTNER)
    names = (expert_ids.T, route_logits.T)
    routed = call(
        routing_kernel, where, names, whole(*names),
        [shape((1, total_tokens), jnp.int32), shape((capacity, 1), jnp.float32), shape((total_tokens, capacity), bf16)],
    )
    line = call(lines_kernel, where, ins, whole(*ins), [shape((2 * RING * own_tokens, half // 2), bf16)] * 2)
    left, right, slots, slot_weight, spread = lax.optimization_barrier((*line, *routed))
    cut = 512
    turned = pl.pallas_call(
        turn_kernel,
        grid_spec=pltpu.PrefetchScalarGridSpec(
            num_scalar_prefetch=1, grid=(width // cut,),
            in_specs=[pl.BlockSpec((units, cut), lambda i, s: (0, i))] * 2,
            out_specs=pl.BlockSpec((cut, 2 * units), lambda i, s: (i, 0)),
        ),
        out_shape=shape((width, 2 * units), bf16),
        compiler_params=LIMIT,
        cost_estimate=pl.CostEstimate(flops=10**9, bytes_accessed=4 * 2**20, transcendentals=0),
    )(where, w_gate[0].T, w_up[0].T)
    blocks, left_far, right_far = relay(1, left, right)
    slots, turned = lax.optimization_barrier((slots, turned))
    ins = (slots, *blocks)
    parts = call(
        dispatch_kernel, where, ins, whole(*ins), [shape((capacity, half // 2), bf16)] * 2, flops=capacity * total_tokens * half
    )
    near_in, far_in = [], []
    for part, block in ((parts[0], left_far), (parts[1], right_far)):
        ins = (slots, part, block)
        near_in += call(finish_kernel, where, ins, whole(*ins), [shape((capacity, half // 2), bf16)], flops=capacity**2 * half)
        far_in.append(lax.ppermute(near_in[-1], "neuron", PARTNER))
    near_half = pl.BlockSpec((half, 2 * units), lambda i, s: (s[0], 0))
    far_half = pl.BlockSpec((half, 2 * units), lambda i, s: (1 - s[0], 0))
    sums = call(
        near_kernel, where, (*near_in, turned), [*whole(*near_in), near_half],
        [shape((capacity, 2 * units), jnp.float32)], flops=4 * capacity * half * units,
    )[0]
    rows = capacity // 2

    def far_rows(which):
        def half_of(span):
            return pl.BlockSpec((rows, span), lambda i, s: (which(s[0]), 0))

        return call(
            far_kernel, where, (*far_in, turned, sums, block_live),
            [half_of(half // 2), half_of(half // 2), far_half, half_of(2 * units), pl.BlockSpec(memory_space=pltpu.SMEM)],
            [shape((rows, units), bf16)], flops=2 * capacity * half * units,
        )[0]

    given = far_rows(lambda c: 1 - c)
    hidden_far = lax.ppermute(given, "neuron", PARTNER)
    hidden = far_rows(lambda c: c)
    ins = (hidden, hidden_far, w_down[0], down_far, slot_weight)
    pieces = {}
    for steps in DOWN_STEPS:
        outs = call(
            functools.partial(down_kernel, steps), where, ins, whole(*ins),
            [shape((rows, width // RING), bf16)] * len(steps), flops=len(steps) * capacity * half * units,
        )
        pieces.update(zip(steps, outs))
    ins = ring(0, pieces, False)
    pieces = {}
    for steps in DOWN_STEPS:
        outs = call(
            functools.partial(middle_kernel, steps), where, ins, whole(*ins), [shape((rows, 2 * col), bf16)] * len(steps)
        )
        pieces.update(zip(steps, outs))
    ins = ring(1, pieces, False)
    given = call(given_kernel, where, ins, whole(*ins), [shape((rows, col), bf16)])[0]
    other = lax.ppermute(given, "neuron", PARTNER)
    ins = (spread, *ins)
    near_placed = call(placed_kernel, where, ins, whole(*ins), [shape((total_tokens, col), jnp.float32)])[0]
    ins = (spread, near_placed, other)
    placed = call(last_kernel, where, ins, whole(*ins), [shape((total_tokens, col), bf16)])[0]
    over = lax.all_to_all(placed, ("expert", "neuron"), 0, 0, tiled=True)
    owned = jnp.sum(over.reshape(planes, members * share, col).astype(jnp.float32), axis=0).astype(bf16)
    copies = jnp.broadcast_to(owned[None], (planes, members * share, col))
    every = lax.all_to_all(copies, "expert", 0, 0, tiled=True)
    every = every.reshape(planes, members, share, col).transpose(0, 2, 1, 3)
    return every.reshape(own_tokens, width)


def solution(mesh):
    placed = (
        P("neuron", None),
        P(),
        P(),
        P("expert", "neuron"),
        P("expert", None, "neuron"),
        P("expert", None, "neuron"),
        P("expert", "neuron", None),
    )

    def body(*args):
        return per_device(mesh.shape["expert"], *args)

    return jax.shard_map(body, mesh=mesh, in_specs=placed, out_specs=P("neuron", None), check_vma=False)
```

```python
import functools

import jax
import jax.numpy as jnp
from jax import lax
from jax.experimental import pallas as pl
from jax.experimental.pallas import tpu as pltpu
from jax.sharding import PartitionSpec as P


BLK = 64
RING = 4


def device(y, x, c):
    return ((y % RING) * RING + x % RING) * 2 + c


PLACES = [(y, x, c) for y in range(RING) for x in range(RING) for c in range(2)]
PARTNER = [(device(y, x, c), device(y, x, 1 - c)) for y, x, c in PLACES]


def turn(d, leg):
    pairs = []
    for y, x, c in PLACES:
        on = device(y, x + d, c) if c == leg else device(y + d, x, c)
        pairs.append((device(y, x, c), on))
    return pairs


def ring(leg, blocks, back):
    got = {0: blocks[0]}
    for d in STEPS:
        pairs = turn(d, leg)
        got[d] = lax.ppermute(blocks[d], "neuron", [(t, s) for s, t in pairs] if back else pairs)
    return [got[k] for k in range(RING)]


def relay(leg, left, right):
    on = turn(1, leg)
    back = [(t, s) for s, t in on]

    def send(value, pairs):
        return lax.ppermute(value, "neuron", pairs)

    left_before, right_after = send(left, on), send(right, back)
    right_before, left_after = send(right, on), send(left, back)
    left_far, right_far = send(left_before, on), send(right_after, back)
    return [left, left_after, left_before, right, right_after, right_before], left_far, right_far


STEPS = (2, 1, 3)
DOWN_STEPS = ((2,), (1, 3), (0,))


def mm(a, b):
    return jnp.dot(a, b, preferred_element_type=jnp.float32)


LIMIT = pltpu.CompilerParams(vmem_limit_bytes=20 * 2**20)


def whole(*arrays):
    return [pl.BlockSpec(a.shape, lambda i, s, n=len(a.shape): (0,) * n) for a in arrays]


def place_of():
    n = lax.axis_index("neuron")
    core, x, y = n & 1, (n >> 1) & (RING - 1), n >> 3
    along_x = core == 0
    return [
        core, lax.axis_index("expert"), jnp.where(along_x, x, y), jnp.where(along_x, y, x),
        jnp.where(along_x, 1, RING), jnp.where(along_x, RING, 1),
    ]


def call(body, place, ins, specs, outs, scratch=(), flops=10**9, steps=1):
    cost = pl.CostEstimate(flops=flops, bytes_accessed=4 * 2**20, transcendentals=0)
    if specs is None:
        def inner(*refs):
            body(place_of(), *refs)

        return pl.pallas_call(
            inner, out_shape=outs, scratch_shapes=list(scratch), compiler_params=LIMIT, cost_estimate=cost
        )(*ins)
    return pl.pallas_call(
        body,
        grid_spec=pltpu.PrefetchScalarGridSpec(
            num_scalar_prefetch=1, grid=(steps,), in_specs=specs, out_specs=whole(*outs), scratch_shapes=list(scratch)
        ),
        out_shape=outs,
        compiler_params=LIMIT,
        cost_estimate=cost,
    )(place, *ins)


def rows_kernel(place, mine, theirs, out):
    rows = mine.shape[0]
    for source, core in ((mine, place[0]), (theirs, 1 - place[0])):
        out[pl.ds(pl.multiple_of(core * rows, rows), rows), :] = source[...]


def copy_kernel(place, source, out):
    out[...] = source[...]


def lines_kernel(place, *refs):
    rows, span = refs[0].shape[0], refs[-1].shape[1]
    for k in range(RING):
        at = pl.ds(pl.multiple_of((place[2] + k) % RING * rows, rows), rows)
        refs[-2][at, :] = refs[k][:, :span]
        refs[-1][at, :] = refs[k][:, span:]


def routing_kernel(place, ids, logits, slots, weight, spread):
    total_tokens, capacity = ids.shape[1], spread.shape[1]
    lanes = 128
    first, second = (jnp.where(ids[k : k + 1, :] == place[1], 1.0, 0.0) for k in range(2))
    lead = 1.0 / (1.0 + jnp.exp(logits[1:2, :] - logits[0:1, :]))
    share = first * lead + second * (1.0 - lead)
    chosen = first + second
    chunks = [chosen[:, k : k + lanes] for k in range(0, total_tokens, lanes)]
    grid = jnp.concatenate(chunks, axis=0)
    earlier = lax.broadcasted_iota(jnp.int32, (lanes, lanes), 0) < lax.broadcasted_iota(jnp.int32, (lanes, lanes), 1)
    before = mm(grid.astype(jnp.bfloat16), jnp.where(earlier, 1.0, 0.0).astype(jnp.bfloat16))
    offset = jnp.zeros((1, 1), jnp.float32)
    out = []
    for k, chunk in enumerate(chunks):
        out.append(jnp.where(chunk > 0.0, before[k : k + 1, :] + offset, float(capacity)))
        offset = offset + jnp.sum(chunk, axis=1, keepdims=True)
    slot = jnp.concatenate(out, axis=1).astype(jnp.int32)
    per_chip = total_tokens // RING // RING
    across = jnp.concatenate(
        [slot[:, (y * RING + x) * per_chip : (y * RING + x + 1) * per_chip] for x in range(RING) for y in range(RING)], axis=1
    )
    slots[...] = jnp.where(place[0] == 0, slot, across)
    hit = slot == lax.broadcasted_iota(jnp.int32, (capacity, total_tokens), 0)
    weight[...] = jnp.sum(jnp.where(hit, share, 0.0), axis=1, keepdims=True)
    planes, own = place_counts(total_tokens)
    rows = spread.shape[0]
    each, part = own // planes, rows // planes
    step = 256
    for top in range(0, rows, step):
        row = lax.broadcasted_iota(jnp.int32, (step, total_tokens), 0) + top
        token = (row % part // each * 2 + place[0]) * own + row // part * each + row % each
        column = lax.broadcasted_iota(jnp.int32, (step, total_tokens), 1)
        mine = jnp.sum(jnp.where(token == column, slot.astype(jnp.float32), 0.0), axis=1, keepdims=True)
        index = lax.broadcasted_iota(jnp.int32, (step, capacity), 1)
        spread[top : top + step, :] = jnp.where(mine.astype(jnp.int32) == index, 1.0, 0.0).astype(jnp.bfloat16)


def place_counts(total_tokens):
    return 8, total_tokens // len(PLACES)


def hot_rows(place, slots, k, capacity, rows):
    line = slots[:, pl.ds(pl.multiple_of((place[3] + k) % RING * rows, rows), rows)]
    index = lax.broadcasted_iota(jnp.int32, (capacity, rows), 0)
    return jnp.where(line == index, 1.0, 0.0).astype(jnp.bfloat16)


def dispatch_kernel(place, slots, *refs):
    outs = refs[-2:]
    rows, span = refs[0].shape
    hot = [hot_rows(place, slots, k, outs[0].shape[0], rows) for k in (0, 1, 3)]
    for side, out in enumerate(outs):
        blocks = refs[3 * side : 3 * side + 3]
        for n in range(0, span, 256):
            acc = mm(hot[0], blocks[0][:, n : n + 256])
            acc = acc + mm(hot[1], blocks[1][:, n : n + 256]) + mm(hot[2], blocks[2][:, n : n + 256])
            out[:, n : n + 256] = acc.astype(jnp.bfloat16)


def finish_kernel(place, slots, part, block, out):
    rows, span = block.shape
    hot = hot_rows(place, slots, 2, out.shape[0], rows)
    for n in range(0, span, 256):
        out[:, n : n + 256] = part[:, n : n + 256] + mm(hot, block[:, n : n + 256]).astype(jnp.bfloat16)


def turn_kernel(place, gate, up, out):
    units = gate.shape[0]
    out[:, :units] = gate[...].T
    out[:, units:] = up[...].T


def near_kernel(place, left, right, both, out):
    cut, units = left.shape[1], out.shape[1]
    for n in range(0, units, 256):
        to = min(n + 256, units)
        out[:, n:to] = mm(left[...], both[:cut, n:to]) + mm(right[...], both[cut:, n:to])


def far_kernel(place, left, right, both, near, live, out):
    cut, units = left.shape[1], out.shape[1]
    block = lax.broadcasted_iota(jnp.int32, (1, units), 1) // BLK
    kept = jnp.zeros((1, units), jnp.float32)
    for k in range(units // BLK):
        kept = jnp.where(block == k, live[0, k].astype(jnp.float32), kept)
    value = near[...] + (mm(left[...], both[:cut, :]) + mm(right[...], both[cut:, :]))
    gate_val, up_val = value[:, :units], value[:, units:]
    out[...] = (gate_val / (1.0 + jnp.exp(-gate_val)) * up_val * kept).astype(jnp.bfloat16)


def down_kernel(steps, place, near, far, w_near, w_far, weight, *outs):
    rows, span = outs[0].shape
    col = span // RING
    scale = weight[pl.ds(pl.multiple_of(place[0] * rows, rows), rows), :]
    for d, out in zip(steps, outs):
        for j in range(RING):
            site = (place[2] + d) % RING * place[4] + j * place[5]
            cols = pl.ds(pl.multiple_of(site * col, col), col)
            value = mm(near[...], w_near[:, cols]) + mm(far[...], w_far[:, cols])
            out[:, j * col : (j + 1) * col] = (value * scale).astype(jnp.bfloat16)


def total_of(refs, block, col):
    cols = pl.ds(pl.multiple_of(block * col, col), col)
    value = refs[0][:, cols].astype(jnp.float32)
    for r in refs[1:]:
        value = value + r[:, cols].astype(jnp.float32)
    return value.astype(jnp.bfloat16)


def middle_kernel(steps, place, *refs):
    got, outs = refs[:RING], refs[RING:]
    for k, out in zip(steps, outs):
        out[...] = total_of(got, (place[3] + k) % RING, out.shape[1])


def mine_kernel(place, *refs):
    value = refs[0][...].astype(jnp.float32)
    for r in refs[1:-1]:
        value = value + r[...].astype(jnp.float32)
    refs[-1][...] = value.astype(jnp.bfloat16)


def placed_kernel(place, spread, mine, out):
    rows = mine.shape[0]
    at = pl.ds(pl.multiple_of(place[0] * rows, rows), rows)
    out[...] = mm(spread[:, at], mine[...])


def last_kernel(place, spread, near, far, out):
    rows = far.shape[0]
    at = pl.ds(pl.multiple_of((1 - place[0]) * rows, rows), rows)
    out[...] = (near[...] + mm(spread[:, at], far[...])).astype(jnp.bfloat16)


def per_device(planes, tokens, route_logits, expert_ids, block_live, w_gate, w_up, w_down):
    total_tokens = expert_ids.shape[0]
    own_tokens, width = tokens.shape
    capacity = total_tokens // 2
    sites = RING * RING
    members = 2 * sites
    share = own_tokens // planes
    half = width // 2
    col = half // sites
    place = lax.axis_index("neuron")
    core, x, y = place % 2, place // 2 % RING, place // (2 * RING)
    along_x = core == 0
    one, two = jnp.where(along_x, x, y), jnp.where(along_x, y, x)
    where = jnp.stack(
        [core, lax.axis_index("expert"), one, two, jnp.where(along_x, 1, RING), jnp.where(along_x, RING, 1)]
    ).astype(jnp.int32)
    where, tokens = lax.optimization_barrier((where, tokens))
    shape = jax.ShapeDtypeStruct
    units = w_gate.shape[2]
    bf16 = jnp.bfloat16

    theirs = lax.ppermute(tokens, "neuron", PARTNER)
    own_half = pl.BlockSpec((own_tokens, half), lambda i, s: (0, s[0]))
    mine = call(copy_kernel, where, (tokens,), [own_half], [shape((own_tokens, half), bf16)])[0]
    chip_rows = call(
        rows_kernel, where, (mine, theirs), [*whole(mine), own_half], [shape((2 * own_tokens, half), bf16)]
    )[0]
    chip_rows, w_down, expert_ids, route_logits = lax.optimization_barrier((chip_rows, w_down, expert_ids, route_logits))
    ins = ring(0, [chip_rows] * RING, True)
    down_far = lax.ppermute(w_down[0], "neuron", PARTNER)
    names = (expert_ids.T, route_logits.T)
    routed = call(
        routing_kernel, where, names, None,
        [shape((1, total_tokens), jnp.int32), shape((capacity, 1), jnp.float32), shape((total_tokens // 2, capacity), bf16)],
    )
    line = call(lines_kernel, where, ins, None, [shape((2 * RING * own_tokens, half // 2), bf16)] * 2)
    left, right, slots, slot_weight, spread = lax.optimization_barrier((*line, *routed))
    cut = 512
    turned = pl.pallas_call(
        turn_kernel,
        grid_spec=pltpu.PrefetchScalarGridSpec(
            num_scalar_prefetch=1, grid=(width // cut,),
            in_specs=[pl.BlockSpec((units, cut), lambda i, s: (0, i))] * 2,
            out_specs=pl.BlockSpec((cut, 2 * units), lambda i, s: (i, 0)),
        ),
        out_shape=shape((width, 2 * units), bf16),
        compiler_params=LIMIT,
        cost_estimate=pl.CostEstimate(flops=10**9, bytes_accessed=4 * 2**20, transcendentals=0),
    )(where, w_gate[0].T, w_up[0].T)
    blocks, left_far, right_far = relay(1, left, right)
    slots, turned = lax.optimization_barrier((slots, turned))
    ins = (slots, *blocks)
    parts = call(
        dispatch_kernel, where, ins, None, [shape((capacity, half // 2), bf16)] * 2, flops=capacity * total_tokens * half
    )
    near_in, far_in = [], []
    for part, block in ((parts[0], left_far), (parts[1], right_far)):
        ins = (slots, part, block)
        near_in += call(finish_kernel, where, ins, None, [shape((capacity, half // 2), bf16)], flops=capacity**2 * half)
        far_in.append(lax.ppermute(near_in[-1], "neuron", PARTNER))
    near_half = pl.BlockSpec((half, 2 * units), lambda i, s: (s[0], 0))
    far_half = pl.BlockSpec((half, 2 * units), lambda i, s: (1 - s[0], 0))
    sums = call(
        near_kernel, where, (*near_in, turned), [*whole(*near_in), near_half],
        [shape((capacity, 2 * units), jnp.float32)], flops=4 * capacity * half * units,
    )[0]
    rows = capacity // 2

    def far_rows(which):
        def half_of(span):
            return pl.BlockSpec((rows, span), lambda i, s: (which(s[0]), 0))

        return call(
            far_kernel, where, (*far_in, turned, sums, block_live),
            [half_of(half // 2), half_of(half // 2), far_half, half_of(2 * units), pl.BlockSpec(memory_space=pltpu.SMEM)],
            [shape((rows, units), bf16)], flops=2 * capacity * half * units,
        )[0]

    given = far_rows(lambda c: 1 - c)
    hidden_far = lax.ppermute(given, "neuron", PARTNER)
    hidden = far_rows(lambda c: c)
    ins = (hidden, hidden_far, w_down[0], down_far, slot_weight)
    pieces = {}
    for steps in DOWN_STEPS:
        outs = call(
            functools.partial(down_kernel, steps), where, ins, None,
            [shape((rows, width // RING), bf16)] * len(steps), flops=len(steps) * capacity * half * units,
        )
        pieces.update(zip(steps, outs))
    ins = ring(0, pieces, False)
    pieces = {}
    for steps in DOWN_STEPS:
        outs = call(
            functools.partial(middle_kernel, steps), where, ins, None, [shape((rows, 2 * col), bf16)] * len(steps)
        )
        pieces.update(zip(steps, outs))
    ins = ring(1, pieces, False)
    mine = call(mine_kernel, where, ins, None, [shape((rows, 2 * col), bf16)])[0]
    other = lax.ppermute(mine, "neuron", PARTNER)
    ins = (spread, mine)
    near_placed = call(placed_kernel, where, ins, None, [shape((total_tokens // 2, 2 * col), jnp.float32)])[0]
    ins = (spread, near_placed, other)
    placed = call(last_kernel, where, ins, None, [shape((total_tokens // 2, 2 * col), bf16)])[0]
    same_core = [[z * members + 2 * s + c for z in range(planes) for s in range(sites)] for c in range(2)]
    over = lax.all_to_all(placed, ("expert", "neuron"), 0, 0, axis_index_groups=same_core, tiled=True)
    owned = jnp.sum(over.reshape(planes, sites * share, 2 * col).astype(jnp.float32), axis=0).astype(bf16)
    copies = jnp.broadcast_to(owned[None], (planes, sites * share, 2 * col))
    every = lax.all_to_all(copies, "expert", 0, 0, tiled=True)
    every = every.reshape(planes, sites, share, 2 * col).transpose(0, 2, 1, 3)
    return every.reshape(own_tokens, width)


def solution(mesh):
    placed = (
        P("neuron", None),
        P(),
        P(),
        P("expert", "neuron"),
        P("expert", None, "neuron"),
        P("expert", None, "neuron"),
        P("expert", "neuron", None),
    )

    def body(*args):
        return per_device(mesh.shape["expert"], *args)

    return jax.shard_map(body, mesh=mesh, in_specs=placed, out_specs=P("neuron", None), check_vma=False)
```
